32 devices in a mesh: tm: 4 (over y, x), space: 8 (over z, core).
Axes of the slice: x: 2, y: 2, z: 4, core: 2. Of those that a mesh axis runs over, the one named last changes fastest.
Arguments:
- positions: float32 [4, 3, 3, 2048], P('tm', None, None, 'space'), may hold values from -4 to 4
- velocities: float32 [4, 3, 3, 2048], P('tm', None, None, 'space'), may hold values from -3 to 3
- masses: float32 [2048], P('space'), may hold values from 0.2 to 2
- initial_places: float32 [3, 2048], P(None, 'space'), may hold values from -4 to 4
- initial_speeds: float32 [3, 2048], P(None, 'space'), may hold values from -3 to 3
Outputs:
- node_places: float32 [4, 2, 3, 2048], P('tm', None, None, 'space')
- node_speeds: float32 [4, 2, 3, 2048], P('tm', None, None, 'space')
- end_force: float32 [4, 3, 2048], P('tm', None, 'space')
- start_places: float32 [4, 3, 2048], P('tm', None, 'space')
- start_speeds: float32 [4, 3, 2048], P('tm', None, 'space')
The draws below stay inside these ranges and needn't reach their ends.
All inputs are finite; a program needn't handle non-finite values.
Results may differ from the reference program's by a relative error of at most 0.0003.
Values sent between devices are 32-bit elements; how exact they have to be, the bound alone decides.
A program may use at most 64 MiB of HBM per device.

```python
import math
import jax
import jax.numpy as jnp
from jax import lax

NODES = 3
BODIES = 2048
SLICES = 4


def shard_levels(rng, extent, split, low, largest):
    level = 1.0
    for position, blocks in split:
        heights = jax.random.uniform(jax.random.fold_in(jax.random.fold_in(rng, 6), position), (blocks,), jnp.float32, low / len(split), largest / len(split))
        level = level * jnp.repeat(jnp.exp(heights), extent[position] // blocks).reshape((-1,) + (1,) * (len(extent) - 1 - position))
    return level


def gaussian(own_key, extent, width, limit, split=(), held_as=jnp.bfloat16):
    entries = jax.random.normal(own_key, extent, jnp.float32) * width
    if len(split) > 0:
        entries = shard_levels(own_key, extent, split, -0.22, 0.18) * entries
    return jnp.clip(entries, min=-limit, max=limit).astype(held_as)


def setup_inputs(seed: int = 0) -> dict:
    key_of = jax.random.split(jax.random.key(seed), 6)
    positions = gaussian(key_of[0], (SLICES, NODES, 3, BODIES), 1.0, 4.0, ((0, 4), (3, 8)), jnp.float32)
    velocities = gaussian(key_of[1], (SLICES, NODES, 3, BODIES), 0.5, 3.0, ((0, 4), (3, 8)), jnp.float32)
    masses = jnp.clip(jnp.exp(math.log(2.0) - 2.3025851 * jax.random.uniform(key_of[2], (BODIES,), jnp.float32) ** shard_levels(key_of[2], (BODIES,), ((0, 8),), -0.2, 0.2)), 0.2, 2.0)
    initial_places = gaussian(key_of[3], (3, BODIES), 1.0, 4.0, ((1, 8),), jnp.float32)
    initial_speeds = gaussian(key_of[4], (3, BODIES), 0.5, 3.0, ((1, 8),), jnp.float32)
    return dict(positions=positions, velocities=velocities, masses=masses, initial_places=initial_places, initial_speeds=initial_speeds)


soften = 0.01
slice_length = 0.25
lobatto_weights = ((5.0 / 24.0, 1.0 / 3.0, -1.0 / 24.0), (-1.0 / 24.0, 1.0 / 3.0, 5.0 / 24.0))

def gravity(places, masses):
    body_count = places.shape[1]
    block = math.gcd(body_count, 512)
    row_blocks = jnp.transpose(places.reshape(3, body_count // block, block), (1, 0, 2))
    weighted = places * masses[None, :]

    def one_block(local_places):
        squared = (places[0][None, :] - local_places[0][:, None]) ** 2
        squared = squared + (places[1][None, :] - local_places[1][:, None]) ** 2
        squared = squared + (places[2][None, :] - local_places[2][:, None]) ** 2
        inverse = lax.rsqrt(squared + soften)
        kernel = inverse * inverse * inverse
        attract = jnp.dot(weighted, kernel.T, precision=lax.Precision.HIGHEST)
        kernel_sum = jnp.dot(masses, kernel.T, precision=lax.Precision.HIGHEST)
        return (attract - local_places * kernel_sum[None, :]) / body_count
    results = lax.map(one_block, row_blocks)
    return jnp.transpose(results, (1, 0, 2)).reshape(3, body_count)

def slice_sweep(places, speeds, masses):
    earlier = [gravity(places[node], masses) for node in range(3)]
    new_places = [places[0]]
    new_speeds = [speeds[0]]
    new_force = [earlier[0]]
    half_step = 0.5 * slice_length
    for node in range(2):
        weights = lobatto_weights[node]
        moved = slice_length * (weights[0] * speeds[0] + weights[1] * speeds[1] + weights[2] * speeds[2])
        kicked = slice_length * (weights[0] * earlier[0] + weights[1] * earlier[1] + weights[2] * earlier[2])
        place = new_places[node] + half_step * (new_speeds[node] - speeds[node]) + moved
        speed = new_speeds[node] + half_step * (new_force[node] - earlier[node]) + kicked
        new_places.append(place)
        new_speeds.append(speed)
        new_force.append(gravity(place, masses))
    drift_place = new_places[2] - (places[0] + slice_length * speeds[0])
    drift_speed = new_speeds[2] - speeds[0]
    return (jnp.stack(new_places[1:]), jnp.stack(new_speeds[1:]), new_force[2], drift_place, drift_speed)

def reference(positions, velocities, masses, initial_places, initial_speeds):

    def per_slice(couple):
        return slice_sweep(couple[0], couple[1], masses)
    node_places, node_speeds, end_force, drift_place, drift_speed = lax.map(per_slice, (positions, velocities))
    carry_place = initial_places
    carry_speed = initial_speeds
    start_list = []
    speed_list = []
    for slice_number in range(SLICES):
        start_list.append(carry_place)
        speed_list.append(carry_speed)
        carry_place = carry_place + slice_length * carry_speed + drift_place[slice_number]
        carry_speed = carry_speed + drift_speed[slice_number]
    return (node_places, node_speeds, end_force, jnp.stack(start_list), jnp.stack(speed_list))
```

```python
import functools
import jax
import jax.numpy as jnp
from jax import lax
from jax.experimental import pallas as pl
from jax.experimental.pallas import tpu as pltpu
from jax.sharding import PartitionSpec as P

soften = 0.01
slice_length = 0.25
lobatto_weights = ((5.0 / 24.0, 1.0 / 3.0, -1.0 / 24.0), (-1.0 / 24.0, 1.0 / 3.0, 5.0 / 24.0))
LANES = 128
MESH = pl.DeviceIdType.MESH
EARLY = 4


def round_up(value, step):
    return (value + step - 1) // step * step


def target_of(me, step, count):
    if count & (count - 1) == 0:
        peer, bit = 0, 1
        while bit < count:
            peer = peer + ((me // bit + step // bit) % 2) * bit
            bit *= 2
        return peer
    return (me + step) % count


def source_of(me, step, count):
    if count & (count - 1) == 0:
        return target_of(me, step, count)
    return (me + count - step) % count


def kernel(
    n, slices, body_count, chunk,
    pos, vel, mass, place0, speed0,
    places_out, speeds_out, force_out, start_out, start_speed_out,
    old, first, last, drift, speeds, own, wide, total, force_rows,
    send_old, recv_old, send_first, recv_first, send_last, recv_last, send_drift, recv_drift,
):
    me = lax.axis_index("space")
    slot = lax.axis_index("tm")
    block = pos.shape[3]
    halves = block // LANES
    rows = 3 * halves
    tile = old.shape[1] // 3

    barrier = pltpu.get_barrier_semaphore()
    for step in range(1, n):
        pl.semaphore_signal(barrier, inc=1, device_id={"space": target_of(me, step, n)}, device_id_type=MESH)
    for step in range(1, slices):
        pl.semaphore_signal(barrier, inc=1, device_id={"tm": (slot + step) % slices}, device_id_type=MESH)

    def lanes_of(half):
        return pl.ds(half * LANES, LANES)

    for comp in range(3):
        for half in range(halves):
            row = comp * halves + half
            for node in range(3):
                old[me, pl.ds(node * tile + row, 1), :] = pos[0, node, pl.ds(comp, 1), lanes_of(half)]
                speeds[node, pl.ds(row, 1), :] = vel[0, node, pl.ds(comp, 1), lanes_of(half)]
            own[0, pl.ds(row, 1), :] = place0[pl.ds(comp, 1), lanes_of(half)]
            own[1, pl.ds(row, 1), :] = speed0[pl.ds(comp, 1), lanes_of(half)]
    for half in range(halves):
        old[me, pl.ds(rows + half, 1), :] = mass[:, lanes_of(half)]

    speed = [speeds[node, pl.ds(0, rows), :] for node in range(3)]
    x0 = old[me, pl.ds(0, rows), :]
    half_step = 0.5 * slice_length

    def moved(weights):
        return slice_length * (weights[0] * speed[0] + weights[1] * speed[1] + weights[2] * speed[2])

    x1 = x0 + half_step * (speed[0] - speed[0]) + moved(lobatto_weights[0])
    first[me, pl.ds(0, rows), :] = x1

    def widen(node, ref, offset):
        for comp in range(3):
            for half in range(halves):
                line = ref[me, pl.ds(offset + comp * halves + half, 1), :]
                wide[node, comp, lanes_of(half), :] = jnp.broadcast_to(line, (LANES, LANES)).T

    def copy(ref, send, recv, step):
        return pltpu.make_async_remote_copy(
            src_ref=ref.at[me], dst_ref=ref.at[me], send_sem=send.at[step], recv_sem=recv.at[step],
            device_id={"space": target_of(me, step, n)}, device_id_type=MESH,
        )

    def arrival(ref, send, recv, step):
        whose = source_of(me, step, n)
        pltpu.make_async_remote_copy(
            src_ref=ref.at[whose], dst_ref=ref.at[whose], send_sem=send.at[step], recv_sem=recv.at[step],
            device_id={"space": target_of(me, step, n)}, device_id_type=MESH,
        ).wait_recv()
        return whose

    def pairs(whose, parts, fresh):
        def one_chunk(index, carry):
            span = pl.ds(pl.multiple_of(index * chunk, chunk), chunk)
            for node, ref, offset in parts:
                here = [wide[node, comp, span, :] for comp in range(3)]
                sums = [None] * 3 if fresh else [total[node, comp, span, :] for comp in range(3)]
                for half in range(halves):
                    gap = [ref[whose, pl.ds(offset + comp * halves + half, 1), :] - here[comp] for comp in range(3)]
                    weight = old[whose, pl.ds(rows + half, 1), :]
                    squared = gap[0] * gap[0] + gap[1] * gap[1] + gap[2] * gap[2]
                    inverse = lax.rsqrt(squared + soften)
                    pull = (inverse * inverse) * (inverse * weight)
                    sums = [pull * gap[comp] if sums[comp] is None else sums[comp] + pull * gap[comp] for comp in range(3)]
                for comp in range(3):
                    total[node, comp, span, :] = sums[comp]
            return carry

        lax.fori_loop(0, block // chunk, one_chunk, 0)

    ones = jnp.ones((8, 2 * LANES), jnp.bfloat16)

    def finish(node):
        sums = total[node].reshape(3 * block, LANES)
        high = sums.astype(jnp.bfloat16)
        low = (sums - high.astype(jnp.float32)).astype(jnp.bfloat16)
        both = jnp.concatenate([high, low], axis=1)
        line = lax.dot_general(ones, both, (((1,), (1,)), ((), ())), preferred_element_type=jnp.float32)
        for row in range(rows):
            force_rows[node, pl.ds(row, 1), :] = line[0:1, row * LANES:(row + 1) * LANES]
        return force_rows[node, pl.ds(0, rows), :] / body_count

    old_parts = [(node, old, node * tile) for node in range(3)]
    first_part = [(3, first, 0)]
    last_part = [(4, last, 0)]

    for node in range(3):
        widen(node, old, node * tile)
    pl.semaphore_wait(barrier, n - 1 + slices - 1)
    for step in range(1, n):
        copy(old, send_old, recv_old, step).start()
    for step in range(1, n):
        copy(first, send_first, recv_first, step).start()
    pairs(me, old_parts, True)
    widen(3, first, 0)
    pairs(me, first_part, True)

    def with_first(step, carry):
        whose = arrival(old, send_old, recv_old, step)
        pairs(whose, old_parts, False)
        return carry

    lax.fori_loop(1, n, with_first, 0)

    a_old = [finish(node) for node in range(3)]

    def kicked(weights):
        return slice_length * (weights[0] * a_old[0] + weights[1] * a_old[1] + weights[2] * a_old[2])

    v0, a0 = speed[0], a_old[0]
    v1 = v0 + half_step * (a0 - a_old[0]) + kicked(lobatto_weights[0])
    x2 = x1 + half_step * (v1 - speed[1]) + moved(lobatto_weights[1])
    last[me, pl.ds(0, rows), :] = x2
    for step in range(1, n):
        copy(last, send_last, recv_last, step).start()

    def only_first(step, carry):
        whose = arrival(first, send_first, recv_first, step)
        pairs(whose, first_part, False)
        return carry

    lax.fori_loop(1, n, only_first, 0)
    a1 = finish(3)
    v2 = v1 + half_step * (a1 - a_old[1]) + kicked(lobatto_weights[1])
    drift_rows = drift.shape[1] // 2
    drift[slot, pl.ds(0, rows), :] = x2 - (x0 + slice_length * v0)
    drift[slot, pl.ds(drift_rows, rows), :] = v2 - v0

    def drift_copy(step, whose, to):
        return pltpu.make_async_remote_copy(
            src_ref=drift.at[whose], dst_ref=drift.at[whose], send_sem=send_drift.at[step], recv_sem=recv_drift.at[step],
            device_id={"tm": to}, device_id_type=MESH,
        )

    for step in range(1, slices):
        drift_copy(step, slot, (slot + step) % slices).start()

    widen(4, last, 0)
    pairs(me, last_part, True)

    def put(ref, lead, value):
        for comp in range(3):
            for half in range(halves):
                row = comp * halves + half
                ref[lead + (pl.ds(comp, 1), lanes_of(half))] = value[row:row + 1, :]

    put(places_out, (0, 0), x1)
    put(places_out, (0, 1), x2)
    put(speeds_out, (0, 0), v1)
    put(speeds_out, (0, 1), v2)

    def only_last(step, carry):
        whose = arrival(last, send_last, recv_last, step)
        pairs(whose, last_part, False)
        return carry

    lax.fori_loop(1, n, only_last, 0)
    a2 = finish(4)
    put(force_out, (0,), a2)

    start_place = own[0, pl.ds(0, rows), :] + slot.astype(jnp.float32) * slice_length * own[1, pl.ds(0, rows), :]
    start_speed = own[1, pl.ds(0, rows), :]
    for step in range(1, slices):
        whose = (slot + slices - step) % slices
        drift_copy(step, whose, whose).wait_recv()
        moved_place = drift[whose, pl.ds(0, rows), :]
        moved_speed = drift[whose, pl.ds(drift_rows, rows), :]
        ahead = (slot - 1 - whose).astype(jnp.float32) * slice_length
        counts = whose < slot
        start_place = start_place + jnp.where(counts, moved_place + ahead * moved_speed, 0.0)
        start_speed = start_speed + jnp.where(counts, moved_speed, 0.0)
    put(start_out, (0,), start_place)
    put(start_speed_out, (0,), start_speed)

    for step in range(1, n):
        copy(old, send_old, recv_old, step).wait_send()
        copy(first, send_first, recv_first, step).wait_send()
        copy(last, send_last, recv_last, step).wait_send()
    for step in range(1, slices):
        drift_copy(step, slot, (slot + step) % slices).wait_send()


def solution(mesh):
    n, slices = mesh.shape["space"], mesh.shape["tm"]

    def body(positions, velocities, masses, initial_places, initial_speeds):
        block = positions.shape[3]
        halves = block // LANES
        tile = round_up(4 * halves, 8)
        part = round_up(3 * halves, 8)
        f32 = jnp.float32
        vmem = pl.BlockSpec(memory_space=pltpu.VMEM)
        dma = pltpu.SemaphoreType.DMA
        return pl.pallas_call(
            functools.partial(kernel, n, slices, float(block * n), 64),
            out_shape=(
                jax.ShapeDtypeStruct((1, 2, 3, block), f32),
                jax.ShapeDtypeStruct((1, 2, 3, block), f32),
                jax.ShapeDtypeStruct((1, 3, block), f32),
                jax.ShapeDtypeStruct((1, 3, block), f32),
                jax.ShapeDtypeStruct((1, 3, block), f32),
            ),
            in_specs=[vmem] * 5,
            out_specs=(vmem,) * 5,
            scratch_shapes=[
                pltpu.VMEM((n, 3 * tile, LANES), f32),
                pltpu.VMEM((n, part, LANES), f32),
                pltpu.VMEM((n, part, LANES), f32),
                pltpu.VMEM((slices, 2 * part, LANES), f32),
                pltpu.VMEM((3, part, LANES), f32),
                pltpu.VMEM((2, part, LANES), f32),
                pltpu.VMEM((5, 3, block, LANES), f32),
                pltpu.VMEM((5, 3, block, LANES), f32),
                pltpu.VMEM((5, part, LANES), f32),
                dma((n,)), dma((n,)), dma((n,)), dma((n,)), dma((n,)), dma((n,)),
                dma((slices,)), dma((slices,)),
            ],
            compiler_params=pltpu.CompilerParams(collective_id=0, has_side_effects=True),
        )(positions, velocities, masses.reshape(1, block), initial_places, initial_speeds)

    return jax.shard_map(
        body,
        mesh=mesh,
        in_specs=(
            P("tm", None, None, "space"),
            P("tm", None, None, "space"),
            P("space"),
            P(None, "space"),
            P(None, "space"),
        ),
        out_specs=(
            P("tm", None, None, "space"),
            P("tm", None, None, "space"),
            P("tm", None, "space"),
            P("tm", None, "space"),
            P("tm", None, "space"),
        ),
        check_vma=False,
    )
```

```python
import functools
import jax
import jax.numpy as jnp
from jax import lax
from jax.experimental import pallas as pl
from jax.experimental.pallas import tpu as pltpu
from jax.sharding import PartitionSpec as P

soften = 0.01
slice_length = 0.25
lobatto_weights = ((5.0 / 24.0, 1.0 / 3.0, -1.0 / 24.0), (-1.0 / 24.0, 1.0 / 3.0, 5.0 / 24.0))
LANES = 128
MESH = pl.DeviceIdType.MESH
EARLY = 4


def round_up(value, step):
    return (value + step - 1) // step * step


def target_of(me, step, count):
    if count & (count - 1) == 0:
        peer, bit = 0, 1
        while bit < count:
            peer = peer + ((me // bit + step // bit) % 2) * bit
            bit *= 2
        return peer
    return (me + step) % count


def source_of(me, step, count):
    if count & (count - 1) == 0:
        return target_of(me, step, count)
    return (me + count - step) % count


def kernel(
    n, slices, body_count, chunk,
    pos, vel, mass, place0, speed0,
    places_out, speeds_out, force_out, start_out, start_speed_out,
    old, first, last, drift, speeds, own, load_sem, wide, total, force_rows,
    send_old, recv_old, send_first, recv_first, send_last, recv_last, send_drift, recv_drift,
):
    me = lax.axis_index("space")
    slot = lax.axis_index("tm")
    halves = mass.shape[0]
    block = halves * LANES
    rows = 3 * halves
    tile = old.shape[1] // 3

    barrier = pltpu.get_barrier_semaphore()
    for step in range(1, n):
        pl.semaphore_signal(barrier, inc=1, device_id={"space": target_of(me, step, n)}, device_id_type=MESH)
    for step in range(1, slices):
        pl.semaphore_signal(barrier, inc=1, device_id={"tm": (slot + step) % slices}, device_id_type=MESH)

    def lanes_of(half):
        return pl.ds(half * LANES, LANES)

    loads = [
        pltpu.make_async_copy(mass.at[:, 0, :], old.at[me, pl.ds(rows, halves), :], load_sem.at[0]),
        pltpu.make_async_copy(place0, own.at[0], load_sem.at[1]),
        pltpu.make_async_copy(speed0, own.at[1], load_sem.at[2]),
    ]
    for node in range(3):
        span = pl.ds(node * rows, rows)
        loads.append(pltpu.make_async_copy(pos.at[span, 0, :], old.at[me, pl.ds(node * tile, rows), :], load_sem.at[3 + node]))
        loads.append(pltpu.make_async_copy(vel.at[span, 0, :], speeds.at[node, pl.ds(0, rows), :], load_sem.at[6 + node]))
    for load in loads:
        load.start()
    for load in loads:
        load.wait()

    speed = [speeds[node, pl.ds(0, rows), :] for node in range(3)]
    x0 = old[me, pl.ds(0, rows), :]
    half_step = 0.5 * slice_length

    def moved(weights):
        return slice_length * (weights[0] * speed[0] + weights[1] * speed[1] + weights[2] * speed[2])

    x1 = x0 + half_step * (speed[0] - speed[0]) + moved(lobatto_weights[0])
    first[me, pl.ds(0, rows), :] = x1

    def widen(node, ref, offset):
        for comp in range(3):
            for half in range(halves):
                line = ref[me, pl.ds(offset + comp * halves + half, 1), :]
                wide[node, comp, lanes_of(half), :] = jnp.broadcast_to(line, (LANES, LANES)).T

    def copy(ref, send, recv, step):
        return pltpu.make_async_remote_copy(
            src_ref=ref.at[me], dst_ref=ref.at[me], send_sem=send.at[step], recv_sem=recv.at[step],
            device_id={"space": target_of(me, step, n)}, device_id_type=MESH,
        )

    def arrival(ref, send, recv, step):
        whose = source_of(me, step, n)
        pltpu.make_async_remote_copy(
            src_ref=ref.at[whose], dst_ref=ref.at[whose], send_sem=send.at[step], recv_sem=recv.at[step],
            device_id={"space": target_of(me, step, n)}, device_id_type=MESH,
        ).wait_recv()
        return whose

    def pairs(whose, parts, fresh):
        def one_chunk(index, carry):
            span = pl.ds(pl.multiple_of(index * chunk, chunk), chunk)
            for node, ref, offset in parts:
                here = [wide[node, comp, span, :] for comp in range(3)]
                sums = [None] * 3 if fresh else [total[node, comp, span, :] for comp in range(3)]
                for half in range(halves):
                    gap = [ref[whose, pl.ds(offset + comp * halves + half, 1), :] - here[comp] for comp in range(3)]
                    weight = old[whose, pl.ds(rows + half, 1), :]
                    squared = gap[0] * gap[0] + gap[1] * gap[1] + gap[2] * gap[2]
                    inverse = lax.rsqrt(squared + soften)
                    pull = (inverse * inverse) * (inverse * weight)
                    sums = [pull * gap[comp] if sums[comp] is None else sums[comp] + pull * gap[comp] for comp in range(3)]
                for comp in range(3):
                    total[node, comp, span, :] = sums[comp]
            return carry

        lax.fori_loop(0, block // chunk, one_chunk, 0)

    ones = jnp.ones((8, 2 * LANES), jnp.bfloat16)

    def finish(node):
        sums = total[node].reshape(3 * block, LANES)
        high = sums.astype(jnp.bfloat16)
        low = (sums - high.astype(jnp.float32)).astype(jnp.bfloat16)
        both = jnp.concatenate([high, low], axis=1)
        line = lax.dot_general(ones, both, (((1,), (1,)), ((), ())), preferred_element_type=jnp.float32)
        for row in range(rows):
            force_rows[node, pl.ds(row, 1), :] = line[0:1, row * LANES:(row + 1) * LANES]
        return force_rows[node, pl.ds(0, rows), :] / body_count

    old_parts = [(node, old, node * tile) for node in range(3)]
    first_part = [(3, first, 0)]
    last_part = [(4, last, 0)]

    for node in range(3):
        widen(node, old, node * tile)
    pl.semaphore_wait(barrier, n - 1 + slices - 1)
    for step in range(1, n):
        copy(old, send_old, recv_old, step).start()
    for step in range(1, n):
        copy(first, send_first, recv_first, step).start()
    pairs(me, old_parts, True)
    widen(3, first, 0)
    pairs(me, first_part, True)

    def with_first(step, carry):
        whose = arrival(old, send_old, recv_old, step)
        pairs(whose, old_parts, False)
        return carry

    lax.fori_loop(1, n, with_first, 0)

    a_old = [finish(node) for node in range(3)]

    def kicked(weights):
        return slice_length * (weights[0] * a_old[0] + weights[1] * a_old[1] + weights[2] * a_old[2])

    v0, a0 = speed[0], a_old[0]
    v1 = v0 + half_step * (a0 - a_old[0]) + kicked(lobatto_weights[0])
    x2 = x1 + half_step * (v1 - speed[1]) + moved(lobatto_weights[1])
    last[me, pl.ds(0, rows), :] = x2
    for step in range(1, n):
        copy(last, send_last, recv_last, step).start()

    def only_first(step, carry):
        whose = arrival(first, send_first, recv_first, step)
        pairs(whose, first_part, False)
        return carry

    lax.fori_loop(1, n, only_first, 0)
    a1 = finish(3)
    v2 = v1 + half_step * (a1 - a_old[1]) + kicked(lobatto_weights[1])
    drift_rows = drift.shape[1] // 2
    drift[slot, pl.ds(0, rows), :] = x2 - (x0 + slice_length * v0)
    drift[slot, pl.ds(drift_rows, rows), :] = v2 - v0

    def drift_copy(step, whose, to):
        return pltpu.make_async_remote_copy(
            src_ref=drift.at[whose], dst_ref=drift.at[whose], send_sem=send_drift.at[step], recv_sem=recv_drift.at[step],
            device_id={"tm": to}, device_id_type=MESH,
        )

    for step in range(1, slices):
        drift_copy(step, slot, (slot + step) % slices).start()

    widen(4, last, 0)
    pairs(me, last_part, True)

    def put(ref, value):
        for row in range(rows):
            ref[row] = value[row:row + 1, :]

    def put_pair(ref, value1, value2):
        for comp in range(3):
            for half in range(halves):
                row = comp * halves + half
                ref[comp, half, 0:1, :] = value1[row:row + 1, :]
                ref[comp, half, 1:2, :] = value2[row:row + 1, :]

    put_pair(places_out, x1, x2)
    put_pair(speeds_out, v1, v2)

    def only_last(step, carry):
        whose = arrival(last, send_last, recv_last, step)
        pairs(whose, last_part, False)
        return carry

    lax.fori_loop(1, n, only_last, 0)
    a2 = finish(4)
    put(force_out, a2)

    def in_rows(value):
        return jnp.concatenate(
            [value[comp:comp + 1, half * LANES:(half + 1) * LANES] for comp in range(3) for half in range(halves)], axis=0
        )

    start_speed = in_rows(own[1])
    start_place = in_rows(own[0]) + slot.astype(jnp.float32) * slice_length * start_speed
    for step in range(1, slices):
        whose = (slot + slices - step) % slices
        drift_copy(step, whose, whose).wait_recv()
        moved_place = drift[whose, pl.ds(0, rows), :]
        moved_speed = drift[whose, pl.ds(drift_rows, rows), :]
        ahead = (slot - 1 - whose).astype(jnp.float32) * slice_length
        counts = whose < slot
        start_place = start_place + jnp.where(counts, moved_place + ahead * moved_speed, 0.0)
        start_speed = start_speed + jnp.where(counts, moved_speed, 0.0)
    put(start_out, start_place)
    put(start_speed_out, start_speed)

    for step in range(1, n):
        copy(old, send_old, recv_old, step).wait_send()
        copy(first, send_first, recv_first, step).wait_send()
        copy(last, send_last, recv_last, step).wait_send()
    for step in range(1, slices):
        drift_copy(step, slot, (slot + step) % slices).wait_send()


def write_out(*refs):
    copies = [pltpu.make_async_copy(refs[i], refs[5 + i], refs[10].at[i]) for i in range(5)]
    for copy in copies:
        copy.start()
    for copy in copies:
        copy.wait()


def solution(mesh):
    n, slices = mesh.shape["space"], mesh.shape["tm"]

    def body(positions, velocities, masses, initial_places, initial_speeds):
        block = positions.shape[3]
        halves = block // LANES
        tile = round_up(4 * halves, 8)
        part = round_up(3 * halves, 8)
        f32 = jnp.float32
        vmem = pl.BlockSpec(memory_space=pltpu.VMEM)
        dma = pltpu.SemaphoreType.DMA
        rows = 3 * halves
        shapes = [(3, halves, 2, LANES)] * 2 + [(rows, 1, LANES)] * 3
        anywhere = pl.BlockSpec(memory_space=pl.ANY)
        outs = pl.pallas_call(
            functools.partial(kernel, n, slices, float(block * n), 64),
            out_shape=tuple(pltpu.VMEM(shape, f32) for shape in shapes),
            in_specs=[anywhere] * 5,
            out_specs=(vmem,) * 5,
            scratch_shapes=[
                pltpu.VMEM((n, 3 * tile, LANES), f32),
                pltpu.VMEM((n, part, LANES), f32),
                pltpu.VMEM((n, part, LANES), f32),
                pltpu.VMEM((slices, 2 * part, LANES), f32),
                pltpu.VMEM((3, part, LANES), f32),
                pltpu.VMEM((2, 3, block), f32),
                dma((9,)),
                pltpu.VMEM((5, 3, block, LANES), f32),
                pltpu.VMEM((5, 3, block, LANES), f32),
                pltpu.VMEM((5, part, LANES), f32),
                dma((n,)), dma((n,)), dma((n,)), dma((n,)), dma((n,)), dma((n,)),
                dma((slices,)), dma((slices,)),
            ],
            compiler_params=pltpu.CompilerParams(collective_id=0, has_side_effects=True),
        )(
            positions.reshape(3 * rows, 1, LANES),
            velocities.reshape(3 * rows, 1, LANES),
            masses.reshape(halves, 1, LANES),
            initial_places,
            initial_speeds,
        )
        outs = pl.pallas_call(
            write_out,
            out_shape=tuple(jax.ShapeDtypeStruct(shape, f32) for shape in shapes),
            in_specs=[vmem] * 5,
            out_specs=(anywhere,) * 5,
            scratch_shapes=[dma((5,))],
        )(*(pltpu.with_memory_space_constraint(part, pltpu.VMEM) for part in outs))
        paired = [part.transpose(2, 0, 1, 3).reshape(1, 2, 3, block) for part in outs[:2]]
        return (*paired, *(part.reshape(1, 3, block) for part in outs[2:]))

    return jax.shard_map(
        body,
        mesh=mesh,
        in_specs=(
            P("tm", None, None, "space"),
            P("tm", None, None, "space"),
            P("space"),
            P(None, "space"),
            P(None, "space"),
        ),
        out_specs=(
            P("tm", None, None, "space"),
            P("tm", None, None, "space"),
            P("tm", None, "space"),
            P("tm", None, "space"),
            P("tm", None, "space"),
        ),
        check_vma=False,
    )
```

```python
import functools
import jax
import jax.numpy as jnp
from jax import lax
from jax.experimental import pallas as pl
from jax.experimental.pallas import tpu as pltpu
from jax.sharding import PartitionSpec as P

soften = 0.01
slice_length = 0.25
lobatto_weights = ((5.0 / 24.0, 1.0 / 3.0, -1.0 / 24.0), (-1.0 / 24.0, 1.0 / 3.0, 5.0 / 24.0))
LANES = 128
MESH = pl.DeviceIdType.MESH
EARLY = 4


def round_up(value, step):
    return (value + step - 1) // step * step


def target_of(me, step, count):
    if count & (count - 1) == 0:
        peer, bit = 0, 1
        while bit < count:
            peer = peer + ((me // bit + step // bit) % 2) * bit
            bit *= 2
        return peer
    return (me + step) % count


def source_of(me, step, count):
    if count & (count - 1) == 0:
        return target_of(me, step, count)
    return (me + count - step) % count


def kernel(
    n, slices, body_count, chunk,
    pos, vel, mass, place0, speed0,
    places_out, speeds_out, force_out, start_out, start_speed_out,
    old, first, last, drift, speeds, own, load_sem, wide, total, force_rows,
    send_old, recv_old, send_first, recv_first, send_last, recv_last, send_drift, recv_drift,
):
    me = lax.axis_index("space")
    slot = lax.axis_index("tm")
    halves = mass.shape[0]
    block = halves * LANES
    rows = 3 * halves
    used = {id(old): 3 * rows + halves, id(first): rows, id(last): rows}

    barrier = pltpu.get_barrier_semaphore()
    for step in range(1, n):
        pl.semaphore_signal(barrier, inc=1, device_id={"space": target_of(me, step, n)}, device_id_type=MESH)
    for step in range(1, slices):
        pl.semaphore_signal(barrier, inc=1, device_id={"tm": (slot + step) % slices}, device_id_type=MESH)

    def lanes_of(half):
        return pl.ds(half * LANES, LANES)

    loads = [
        pltpu.make_async_copy(mass.at[:, 0, :], old.at[me, pl.ds(3 * rows, halves), :], load_sem.at[0]),
        pltpu.make_async_copy(place0, own.at[0], load_sem.at[1]),
        pltpu.make_async_copy(speed0, own.at[1], load_sem.at[2]),
    ]
    for node in range(3):
        span = pl.ds(node * rows, rows)
        loads.append(pltpu.make_async_copy(pos.at[span, 0, :], old.at[me, pl.ds(node * rows, rows), :], load_sem.at[3 + node]))
        loads.append(pltpu.make_async_copy(vel.at[span, 0, :], speeds.at[node, pl.ds(0, rows), :], load_sem.at[6 + node]))
    for load in loads:
        load.start()
    for load in loads:
        load.wait()

    speed = [speeds[node, pl.ds(0, rows), :] for node in range(3)]
    x0 = old[me, pl.ds(0, rows), :]
    half_step = 0.5 * slice_length

    def moved(weights):
        return slice_length * (weights[0] * speed[0] + weights[1] * speed[1] + weights[2] * speed[2])

    x1 = x0 + half_step * (speed[0] - speed[0]) + moved(lobatto_weights[0])
    first[me, pl.ds(0, rows), :] = x1

    def widen(node, ref, offset):
        for comp in range(3):
            for half in range(halves):
                line = ref[me, pl.ds(offset + comp * halves + half, 1), :]
                wide[node, comp, lanes_of(half), :] = jnp.broadcast_to(line, (LANES, LANES)).T

    def copy(ref, send, recv, step):
        return pltpu.make_async_remote_copy(
            src_ref=ref.at[me, pl.ds(0, used[id(ref)]), :], dst_ref=ref.at[me, pl.ds(0, used[id(ref)]), :], send_sem=send.at[step], recv_sem=recv.at[step],
            device_id={"space": target_of(me, step, n)}, device_id_type=MESH,
        )

    def arrival(ref, send, recv, step):
        whose = source_of(me, step, n)
        pltpu.make_async_remote_copy(
            src_ref=ref.at[whose, pl.ds(0, used[id(ref)]), :], dst_ref=ref.at[whose, pl.ds(0, used[id(ref)]), :], send_sem=send.at[step], recv_sem=recv.at[step],
            device_id={"space": target_of(me, step, n)}, device_id_type=MESH,
        ).wait_recv()
        return whose

    def pairs(whose, parts, fresh):
        def one_chunk(index, carry):
            span = pl.ds(pl.multiple_of(index * chunk, chunk), chunk)
            for node, ref, offset in parts:
                here = [wide[node, comp, span, :] for comp in range(3)]
                sums = [None] * 3 if fresh else [total[node, comp, span, :] for comp in range(3)]
                for half in range(halves):
                    gap = [ref[whose, pl.ds(offset + comp * halves + half, 1), :] - here[comp] for comp in range(3)]
                    weight = old[whose, pl.ds(3 * rows + half, 1), :]
                    squared = gap[0] * gap[0] + gap[1] * gap[1] + gap[2] * gap[2]
                    inverse = lax.rsqrt(squared + soften)
                    pull = (inverse * inverse) * (inverse * weight)
                    sums = [pull * gap[comp] if sums[comp] is None else sums[comp] + pull * gap[comp] for comp in range(3)]
                for comp in range(3):
                    total[node, comp, span, :] = sums[comp]
            return carry

        lax.fori_loop(0, block // chunk, one_chunk, 0)

    ones = jnp.ones((8, 2 * LANES), jnp.bfloat16)

    def finish(node):
        sums = total[node].reshape(3 * block, LANES)
        high = sums.astype(jnp.bfloat16)
        low = (sums - high.astype(jnp.float32)).astype(jnp.bfloat16)
        both = jnp.concatenate([high, low], axis=1)
        line = lax.dot_general(ones, both, (((1,), (1,)), ((), ())), preferred_element_type=jnp.float32)
        for row in range(rows):
            force_rows[node, pl.ds(row, 1), :] = line[0:1, row * LANES:(row + 1) * LANES]
        return force_rows[node, pl.ds(0, rows), :] / body_count

    old_parts = [(node, old, node * rows) for node in range(3)]
    first_part = [(3, first, 0)]
    last_part = [(4, last, 0)]

    pl.semaphore_wait(barrier, n - 1 + slices - 1)
    for step in range(1, n):
        copy(old, send_old, recv_old, step).start()
    for step in range(1, n):
        copy(first, send_first, recv_first, step).start()
    for node in range(3):
        widen(node, old, node * rows)
    pairs(me, old_parts, True)
    widen(3, first, 0)
    pairs(me, first_part, True)

    def with_first(step, carry):
        whose = arrival(old, send_old, recv_old, step)
        pairs(whose, old_parts, False)
        return carry

    lax.fori_loop(1, n, with_first, 0)

    a_old = [finish(node) for node in range(3)]

    def kicked(weights):
        return slice_length * (weights[0] * a_old[0] + weights[1] * a_old[1] + weights[2] * a_old[2])

    v0, a0 = speed[0], a_old[0]
    v1 = v0 + half_step * (a0 - a_old[0]) + kicked(lobatto_weights[0])
    x2 = x1 + half_step * (v1 - speed[1]) + moved(lobatto_weights[1])
    last[me, pl.ds(0, rows), :] = x2
    for step in range(1, n):
        copy(last, send_last, recv_last, step).start()

    def only_first(step, carry):
        whose = arrival(first, send_first, recv_first, step)
        pairs(whose, first_part, False)
        return carry

    lax.fori_loop(1, n, only_first, 0)
    a1 = finish(3)
    v2 = v1 + half_step * (a1 - a_old[1]) + kicked(lobatto_weights[1])
    drift_rows = drift.shape[1] // 2
    drift[slot, pl.ds(0, rows), :] = x2 - (x0 + slice_length * v0)
    drift[slot, pl.ds(drift_rows, rows), :] = v2 - v0

    def drift_copy(step, whose, to):
        return pltpu.make_async_remote_copy(
            src_ref=drift.at[whose], dst_ref=drift.at[whose], send_sem=send_drift.at[step], recv_sem=recv_drift.at[step],
            device_id={"tm": to}, device_id_type=MESH,
        )

    for step in range(1, slices):
        drift_copy(step, slot, (slot + step) % slices).start()

    widen(4, last, 0)
    pairs(me, last_part, True)

    def put(ref, value):
        for row in range(rows):
            ref[row] = value[row:row + 1, :]

    def put_pair(ref, value1, value2):
        for comp in range(3):
            for half in range(halves):
                row = comp * halves + half
                ref[comp, half, 0:1, :] = value1[row:row + 1, :]
                ref[comp, half, 1:2, :] = value2[row:row + 1, :]

    put_pair(places_out, x1, x2)
    put_pair(speeds_out, v1, v2)

    def only_last(step, carry):
        whose = arrival(last, send_last, recv_last, step)
        pairs(whose, last_part, False)
        return carry

    lax.fori_loop(1, n, only_last, 0)
    a2 = finish(4)
    put(force_out, a2)

    def in_rows(value):
        return jnp.concatenate(
            [value[comp:comp + 1, half * LANES:(half + 1) * LANES] for comp in range(3) for half in range(halves)], axis=0
        )

    start_speed = in_rows(own[1])
    start_place = in_rows(own[0]) + slot.astype(jnp.float32) * slice_length * start_speed
    for step in range(1, slices):
        whose = (slot + slices - step) % slices
        drift_copy(step, whose, whose).wait_recv()
        moved_place = drift[whose, pl.ds(0, rows), :]
        moved_speed = drift[whose, pl.ds(drift_rows, rows), :]
        ahead = (slot - 1 - whose).astype(jnp.float32) * slice_length
        counts = whose < slot
        start_place = start_place + jnp.where(counts, moved_place + ahead * moved_speed, 0.0)
        start_speed = start_speed + jnp.where(counts, moved_speed, 0.0)
    put(start_out, start_place)
    put(start_speed_out, start_speed)

    for step in range(1, n):
        copy(old, send_old, recv_old, step).wait_send()
        copy(first, send_first, recv_first, step).wait_send()
        copy(last, send_last, recv_last, step).wait_send()
    for step in range(1, slices):
        drift_copy(step, slot, (slot + step) % slices).wait_send()


def write_out(*refs):
    copies = [pltpu.make_async_copy(refs[i], refs[5 + i], refs[10].at[i]) for i in range(5)]
    for copy in copies:
        copy.start()
    for copy in copies:
        copy.wait()


def solution(mesh):
    n, slices = mesh.shape["space"], mesh.shape["tm"]

    def body(positions, velocities, masses, initial_places, initial_speeds):
        block = positions.shape[3]
        halves = block // LANES
        packed = round_up(10 * halves, 8)
        part = round_up(3 * halves, 8)
        f32 = jnp.float32
        vmem = pl.BlockSpec(memory_space=pltpu.VMEM)
        dma = pltpu.SemaphoreType.DMA
        rows = 3 * halves
        shapes = [(3, halves, 2, LANES)] * 2 + [(rows, 1, LANES)] * 3
        anywhere = pl.BlockSpec(memory_space=pl.ANY)
        outs = pl.pallas_call(
            functools.partial(kernel, n, slices, float(block * n), 64),
            out_shape=tuple(pltpu.VMEM(shape, f32) for shape in shapes),
            in_specs=[anywhere] * 5,
            out_specs=(vmem,) * 5,
            scratch_shapes=[
                pltpu.VMEM((n, packed, LANES), f32),
                pltpu.VMEM((n, part, LANES), f32),
                pltpu.VMEM((n, part, LANES), f32),
                pltpu.VMEM((slices, 2 * part, LANES), f32),
                pltpu.VMEM((3, part, LANES), f32),
                pltpu.VMEM((2, 3, block), f32),
                dma((9,)),
                pltpu.VMEM((5, 3, block, LANES), f32),
                pltpu.VMEM((5, 3, block, LANES), f32),
                pltpu.VMEM((5, part, LANES), f32),
                dma((n,)), dma((n,)), dma((n,)), dma((n,)), dma((n,)), dma((n,)),
                dma((slices,)), dma((slices,)),
            ],
            compiler_params=pltpu.CompilerParams(collective_id=0, has_side_effects=True),
        )(
            positions.reshape(3 * rows, 1, LANES),
            velocities.reshape(3 * rows, 1, LANES),
            masses.reshape(halves, 1, LANES),
            initial_places,
            initial_speeds,
        )
        outs = pl.pallas_call(
            write_out,
            out_shape=tuple(jax.ShapeDtypeStruct(shape, f32) for shape in shapes),
            in_specs=[vmem] * 5,
            out_specs=(anywhere,) * 5,
            scratch_shapes=[dma((5,))],
        )(*(pltpu.with_memory_space_constraint(part, pltpu.VMEM) for part in outs))
        paired = [part.transpose(2, 0, 1, 3).reshape(1, 2, 3, block) for part in outs[:2]]
        return (*paired, *(part.reshape(1, 3, block) for part in outs[2:]))

    return jax.shard_map(
        body,
        mesh=mesh,
        in_specs=(
            P("tm", None, None, "space"),
            P("tm", None, None, "space"),
            P("space"),
            P(None, "space"),
            P(None, "space"),
        ),
        out_specs=(
            P("tm", None, None, "space"),
            P("tm", None, None, "space"),
            P("tm", None, "space"),
            P("tm", None, "space"),
            P("tm", None, "space"),
        ),
        check_vma=False,
    )
```
